512 devices in a mesh: row: 16 (over y, core), col: 32 (over x, z).
Axes of the slice: x: 4, y: 8, z: 8, core: 2. Of those that a mesh axis runs over, the one named last changes fastest.
Arguments:
- lhat: float32 [4096, 256, 256], P(('row', 'col')), may hold values from -0.375 to 0.375
- ainv_anc: float32 [4096, 256, 256], P(('row', 'col')), may hold values from -1.25 to 1.25
- diag_inv: float32 [32, 256, 256], P('col', 'row'), may hold values from -0.6 to 2, as said below
- targets: int32 [4096, 1], P(('row', 'col')), may hold values from 0 to 31
Outputs:
- diag_blocks: float32 [32, 256, 256], P('col', 'row')
The draws below stay inside these ranges and needn't reach their ends.
Inputs may be any that keep to these rules, and one draw needn't show every extreme that they name: `diag_inv`: each block is lower triangular with its diagonal entries between 0.5 and 2.
All inputs are finite; a program needn't handle non-finite values.
Results may differ from the reference program's by a relative error of at most 0.0003.
Values sent between devices are 32-bit elements; how exact they have to be, the bound alone decides.
No kernel may reach another device: no remote copies, remote signals or barrier semaphores. Data moves between devices by JAX's collectives and lax.ppermute only.
A program may use at most 64 MiB of HBM per device.

```python
import jax
import jax.numpy as jnp
from jax import lax

W = 256
H = 256
SN_DEV = 1
SLOT_DEV = 8
SUPER = 32
SLOTS = 4096
N_ROW = 16
N_COL = 32


def draw_diag_inv(key, part):
    first, second = jax.random.split(jax.random.fold_in(key, 17))
    spread = 0.1 * jax.random.normal(first, (SUPER, W, W), jnp.float32)
    spread = jnp.clip(spread, -0.6, 0.6)
    diagonal = jax.random.uniform(second, (SUPER, W), jnp.float32, 0.5, 2.0)
    lower = jnp.tril(spread, -1)
    return lower + diagonal[:, :, None] * jnp.eye(W, dtype=jnp.float32)[None, :, :]


def steps_of(key, extent, shards, least, high):
    factor_of = 1.0
    for dim, shards_of in shards:
        heights = jax.random.uniform(jax.random.fold_in(jax.random.fold_in(key, 6), dim), (shards_of,), jnp.float32, least / len(shards), high / len(shards))
        factor_of = factor_of * jnp.repeat(jnp.exp(heights), extent[dim] // shards_of).reshape((-1,) + (1,) * (len(extent) - 1 - dim))
    return factor_of


def picks_of(own_key, rows, number_of, top, lift):
    ranking = jax.random.permutation(jax.random.fold_in(own_key, 1), number_of)
    boost = ranking
    for power in range(3):
        boost = boost * boost // number_of
    boost = boost * lift // number_of
    tickets = jax.random.randint(jax.random.fold_in(own_key, 2), (rows, number_of), 0, 4096) + boost
    sure = jax.random.permutation(jax.random.fold_in(own_key, 3), rows)[jnp.arange(number_of) % rows]
    tickets = jnp.where(jnp.arange(rows)[:, None] == sure[None, :], 1 << 14, tickets)
    priority = tickets * number_of + jnp.arange(number_of)
    return lax.top_k(priority.astype(jnp.int32), top)[1].astype(jnp.int32)


def normal_values(stream_key, extent, width, bound, shards=(), held_as=jnp.bfloat16):
    drawn = width * jax.random.normal(stream_key, extent, jnp.float32)
    if shards:
        drawn = drawn * steps_of(stream_key, extent, shards, -0.22, 0.18)
    return jnp.clip(drawn, -bound, bound).astype(held_as)


def setup_inputs(seed: int = 0) -> dict:
    key_of = jax.random.split(jax.random.key(seed), 5)
    lhat = normal_values(key_of[0], (SLOTS, H, W), H ** -0.5, 0.375, ((0, 512),), jnp.float32)
    ainv_anc = normal_values(key_of[1], (SLOTS, H, W), ((SN_DEV / (SLOT_DEV * N_ROW)) ** 0.5), 1.25, ((0, 512),), jnp.float32)
    diag_inv = draw_diag_inv(jax.random.fold_in(key_of[4], 71), 0)
    targets = picks_of(key_of[3], SLOTS, SUPER, 1, 512)
    return dict(lhat=lhat, ainv_anc=ainv_anc, diag_inv=diag_inv, targets=targets)


def reference(lhat, ainv_anc, diag_inv, targets):
    group_size = SLOT_DEV * N_COL
    slot_ids = targets[:, 0].reshape(N_ROW, group_size)
    left_all = lhat.reshape(N_ROW, group_size, H, W)
    right_all = ainv_anc.reshape(N_ROW, group_size, H, W)
    labels = jnp.arange(SN_DEV * N_COL, dtype=jnp.int32)

    def accumulate(running, inputs):
        left_blk, right_blk, ids_blk = inputs
        products = jnp.einsum('shi,shj->sij', left_blk, right_blk, precision=lax.Precision.HIGHEST)
        one_hot = (labels[:, None] == ids_blk[None, :]).astype(jnp.float32)
        added = jnp.einsum('ks,sij->kij', one_hot, products, precision=lax.Precision.HIGHEST)
        return running + added, None

    start_sum = jnp.zeros((SN_DEV * N_COL, W, W), jnp.float32)
    contrib, leftover = lax.scan(accumulate, start_sum, (left_all, right_all, slot_ids))
    gram_term = jnp.einsum('kia,kib->kab', diag_inv, diag_inv, precision=lax.Precision.HIGHEST)
    return gram_term - contrib
```

```python
import jax
import jax.numpy as jnp
from jax import lax
from jax.sharding import PartitionSpec as P

NY, NC, NX, NZ = 8, 2, 4, 8
BOTH = ("row", "col")


def flat(y, c, x, z):
    return ((y * NC + c) * NX + x) * NZ + z


def every():
    return [(y, c, x, z) for y in range(NY) for c in range(NC) for x in range(NX) for z in range(NZ)]


LINES = [[flat(y, 0, x, z) for y in range(NY)] for x in range(NX) for z in range(NZ)] + [
    [flat(y, 1, x, z) for z in range(NZ)] for x in range(NX) for y in range(NY)
]
PLANES = [[flat(y, 0, x, z) for x in range(NX) for z in range(NZ)] for y in range(NY)] + [
    [flat(y, 1, x, z) for x in range(NX) for y in range(NY)] for z in range(NZ)
]
PARTNER = [(flat(y, c, x, z), flat(y, 1 - c, x, z)) for y, c, x, z in every()]
TO_ODD = [(flat(y, 0, x, z), flat(y, 1, x, z)) for y, c, x, z in every() if c == 0]
TURN = [(flat(y, 1, x, z), flat(z, 1, x, y)) for y, c, x, z in every() if c == 1]


def on_device(lhat, ainv_anc, diag_inv, targets):
    slots, _, width = lhat.shape
    core = lax.axis_index("row") % NC
    y = lax.axis_index("row") // NC
    supers = NX * NZ
    share = width // (NY * NC)
    labels = jnp.arange(supers, dtype=jnp.int32)

    ids = targets[:, 0].astype(jnp.float32)
    ids_row = jnp.zeros((8, width), jnp.float32).at[:, :slots].set(ids[None, :])
    mine = jnp.concatenate([diag_inv[0], ids_row], axis=0)
    theirs = lax.ppermute(mine, BOTH, PARTNER)

    def product(side):
        left = lhat.reshape(slots, width, NY, NC, share)
        left = lax.dynamic_index_in_dim(left, side, 3, keepdims=False)
        return jnp.einsum("shdr,shj->dsrj", left, ainv_anc, precision=lax.Precision.HIGH)

    sent = product(1 - core)
    arrived = lax.ppermute(sent, BOTH, PARTNER)
    kept = product(core)
    extra = jnp.concatenate([mine[:share], theirs[:share], mine[share:], theirs[share:]], axis=0)
    payload = jnp.concatenate(
        [
            kept.reshape(NY, slots * share, width),
            arrived.reshape(NY, slots * share, width),
            jnp.broadcast_to(extra[None], (NY, *extra.shape)),
        ],
        axis=1,
    )
    got = lax.all_to_all(payload, BOTH, 0, 0, axis_index_groups=LINES, tiled=True)
    n = NC * slots
    blocks = got[:, : n * share].reshape(NY * n, share, width)
    base = n * share + NC * share
    ids_all = jnp.stack([got[:, base, :slots], got[:, base + 8, :slots]], axis=1).reshape(-1)
    one_hot = (labels[:, None].astype(jnp.float32) == ids_all[None, :]).astype(jnp.float32)
    summed = jnp.einsum("kn,nij->kij", one_hot, blocks, precision=lax.Precision.HIGH)

    factor = got[:, n * share : base].reshape(NY * NC * share, width)
    piece = lax.dynamic_slice_in_dim(factor, y * NC * share, NC * share, 1)
    gram = jnp.einsum("ia,ib->ab", piece, factor, precision=lax.Precision.HIGH)
    gram_odd = lax.ppermute(gram[share:], BOTH, TO_ODD)

    parts = lax.all_to_all(summed, BOTH, 0, 0, axis_index_groups=PLANES, tiled=True)
    own = jnp.sum(parts, axis=0)
    turned = lax.ppermute(own, BOTH, TURN)
    return jnp.where(core == 0, gram[:share] - own, gram_odd - turned)[None]


def solution(mesh):
    placed = (
        P(("row", "col"), None, None),
        P(("row", "col"), None, None),
        P("col", "row", None),
        P(("row", "col"), None),
    )
    return jax.shard_map(
        on_device, mesh=mesh, in_specs=placed, out_specs=P("col", "row", None), check_vma=False
    )
```

```python
import jax
import jax.numpy as jnp
from jax import lax
from jax.experimental import pallas as pl
from jax.experimental.pallas import tpu as pltpu
from jax.sharding import PartitionSpec as P

NY, NC, NX, NZ = 8, 2, 4, 8
BOTH = ("row", "col")


def flat(y, c, x, z):
    return ((y * NC + c) * NX + x) * NZ + z


def every():
    return [(y, c, x, z) for y in range(NY) for c in range(NC) for x in range(NX) for z in range(NZ)]


LINES = [[flat(y, 0, x, z) for y in range(NY)] for x in range(NX) for z in range(NZ)] + [
    [flat(y, 1, x, z) for z in range(NZ)] for x in range(NX) for y in range(NY)
]
PLANES = [[flat(y, 0, x, z) for x in range(NX) for z in range(NZ)] for y in range(NY)] + [
    [flat(y, 1, x, z) for x in range(NX) for y in range(NY)] for z in range(NZ)
]
PARTNER = [(flat(y, c, x, z), flat(y, 1 - c, x, z)) for y, c, x, z in every()]
TO_ODD = [(flat(y, 0, x, z), flat(y, 1, x, z)) for y, c, x, z in every() if c == 0]
TURN = [(flat(y, 1, x, z), flat(z, 1, x, y)) for y, c, x, z in every() if c == 1]


def split(a):
    high = a.astype(jnp.bfloat16)
    return high, (a - high.astype(jnp.float32)).astype(jnp.bfloat16)


def transposed_times(a, b):
    ah, al = split(a.T)
    bh, bl = split(b)
    left = jnp.concatenate([ah, ah, al], axis=1)
    right = jnp.concatenate([bh, bl, bh], axis=0)
    return jnp.dot(left, right, preferred_element_type=jnp.float32)


def products_kernel(where_ref, ids_ref, left_ref, right_ref, rows_ref, kept_ref, sent_ref):
    step = pl.program_id(0)
    core = where_ref[0]
    slots = pl.num_programs(0) - 1
    share, width = rows_ref.shape[1:]

    @pl.when(step < slots)
    def _():
        product = transposed_times(left_ref[0], right_ref[0]).reshape(NY, NC, share, width)
        even, odd = product[:, 0], product[:, 1]
        kept_ref[:, 0] = jnp.where(core == 0, even, odd)
        sent_ref[...] = jnp.where(core == 0, odd, even)

    @pl.when(step == slots)
    def _():
        first = share * where_ref[1] + 1
        row = lax.broadcasted_iota(jnp.int32, (share, width), 0)
        lane = lax.broadcasted_iota(jnp.int32, (share, width), 1)
        tile = jnp.where(lane < first + row, rows_ref[0], 0.0)
        for s in range(ids_ref.shape[0]):
            tile = jnp.where((row == 0) & (lane == first + s), ids_ref[s, 0].astype(jnp.float32), tile)
        tiles = jnp.broadcast_to(tile[None], (NY, share, width))
        kept_ref[:, 0] = tiles
        sent_ref[...] = tiles


def place_kernel(_, arrived_ref, out_ref, sem):
    copy = pltpu.make_async_copy(arrived_ref, out_ref.at[:, 1], sem)
    copy.start()
    copy.wait()


def sum_kernel(where_ref, ids_ref, got_ref, out_ref, factor_ref):
    step = pl.program_id(0)
    core, index = where_ref[0], where_ref[1]
    share = out_ref.shape[1]
    slots = got_ref.shape[2] // share - 1

    @pl.when(step == 0)
    def _():
        out_ref[...] = jnp.zeros_like(out_ref)

    for half in range(NC):
        source_core = core if half == 0 else 1 - core
        source_y = jnp.where(core == 0, step, index // NC)
        first = share * (source_y * NC + source_core) + 1
        for s in range(slots):
            k = ids_ref[0, half, 0, first + s].astype(jnp.int32)
            out_ref[k] += got_ref[0, half, s * share : (s + 1) * share]
        tile = got_ref[0, half, slots * share :]
        row = lax.broadcasted_iota(jnp.int32, tile.shape, 0)
        lane = lax.broadcasted_iota(jnp.int32, tile.shape, 1)
        factor_ref[half * share : (half + 1) * share] = jnp.where(lane < first + row, tile, 0.0)


def gram_kernel(where_ref, factor_ref, out_ref, whole_ref):
    whole_ref[...] = transposed_times(factor_ref[...], factor_ref[...])
    height = out_ref.shape[0]
    out_ref[...] = whole_ref[pl.ds(pl.multiple_of(where_ref[1] // NC * height, height), height)]


def on_device(lhat, ainv_anc, diag_inv, targets):
    slots, height, width = lhat.shape
    index = lax.axis_index("row")
    core = index % NC
    share = diag_inv.shape[1]
    supers = NX * NZ
    length = (slots + 1) * share
    where = jnp.stack([core, index]).astype(jnp.int32)
    smem = pl.BlockSpec(memory_space=pltpu.SMEM)

    kept, sent = pl.pallas_call(
        products_kernel,
        grid=(slots + 1,),
        in_specs=[
            smem,
            smem,
            pl.BlockSpec((1, height, width), lambda i: (jnp.minimum(i, slots - 1), 0, 0)),
            pl.BlockSpec((1, height, width), lambda i: (jnp.minimum(i, slots - 1), 0, 0)),
            pl.BlockSpec((1, share, width), lambda i: (0, 0, 0)),
        ],
        out_specs=[
            pl.BlockSpec((NY, 1, share, width), lambda i: (0, 0, i, 0)),
            pl.BlockSpec((NY, share, width), lambda i: (0, i, 0)),
        ],
        out_shape=[
            jax.ShapeDtypeStruct((NY, NC, length, width), jnp.float32),
            jax.ShapeDtypeStruct((NY, length, width), jnp.float32),
        ],
        name="products",
    )(where, targets, lhat, ainv_anc, diag_inv)

    arrived = lax.ppermute(sent, BOTH, PARTNER)
    payload = pl.pallas_call(
        place_kernel,
        in_specs=[pl.BlockSpec(memory_space=pl.ANY), pl.BlockSpec(memory_space=pltpu.VMEM)],
        out_specs=pl.BlockSpec(memory_space=pl.ANY),
        out_shape=jax.ShapeDtypeStruct(kept.shape, jnp.float32),
        scratch_shapes=[pltpu.SemaphoreType.DMA],
        input_output_aliases={0: 0},
        name="place",
    )(kept, arrived)

    got = lax.all_to_all(payload, BOTH, 0, 0, axis_index_groups=LINES, tiled=True)

    summed, factor = pl.pallas_call(
        sum_kernel,
        grid=(NY,),
        in_specs=[
            smem,
            pl.BlockSpec((1, NC, 8, width), lambda i: (i, 0, slots * share // 8, 0), memory_space=pltpu.SMEM),
            pl.BlockSpec((1, NC, length, width), lambda i: (i, 0, 0, 0)),
        ],
        out_specs=[
            pl.BlockSpec((supers, share, width), lambda i: (0, 0, 0)),
            pl.BlockSpec((NC * share, width), lambda i: (i, 0)),
        ],
        out_shape=[
            jax.ShapeDtypeStruct((supers, share, width), jnp.float32),
            jax.ShapeDtypeStruct((NY * NC * share, width), jnp.float32),
        ],
        name="sum",
    )(where, got, got)

    gram = pl.pallas_call(
        gram_kernel,
        in_specs=[smem, pl.BlockSpec(memory_space=pltpu.VMEM)],
        out_specs=pl.BlockSpec(memory_space=pltpu.VMEM),
        out_shape=jax.ShapeDtypeStruct((NC * share, width), jnp.float32),
        scratch_shapes=[pltpu.VMEM((width, width), jnp.float32)],
        name="gram",
    )(where, factor)
    gram_odd = lax.ppermute(gram[share:], BOTH, TO_ODD)

    parts = lax.all_to_all(summed, BOTH, 0, 0, axis_index_groups=PLANES, tiled=True)
    own = jnp.sum(parts, axis=0)
    turned = lax.ppermute(own, BOTH, TURN)
    return jnp.where(core == 0, gram[:share] - own, gram_odd - turned)[None]


def solution(mesh):
    placed = (
        P(("row", "col"), None, None),
        P(("row", "col"), None, None),
        P("col", "row", None),
        P(("row", "col"), None),
    )
    return jax.shard_map(
        on_device, mesh=mesh, in_specs=placed, out_specs=P("col", "row", None), check_vma=False
    )
```

```python
import jax
import jax.numpy as jnp
from jax import lax
from jax.experimental import pallas as pl
from jax.experimental.pallas import tpu as pltpu
from jax.sharding import PartitionSpec as P

NY, NC, NX, NZ = 8, 2, 4, 8
BOTH = ("row", "col")


def flat(y, c, x, z):
    return ((y * NC + c) * NX + x) * NZ + z


def every():
    return [(y, c, x, z) for y in range(NY) for c in range(NC) for x in range(NX) for z in range(NZ)]


LINES = [[flat(y, 0, x, z) for y in range(NY)] for x in range(NX) for z in range(NZ)] + [
    [flat(y, 1, x, z) for z in range(NZ)] for x in range(NX) for y in range(NY)
]
PLANES = [[flat(y, 0, x, z) for x in range(NX) for z in range(NZ)] for y in range(NY)] + [
    [flat(y, 1, x, z) for x in range(NX) for y in range(NY)] for z in range(NZ)
]
PARTNER = [(flat(y, c, x, z), flat(y, 1 - c, x, z)) for y, c, x, z in every()]
TO_ODD = [(flat(y, 0, x, z), flat(y, 1, x, z)) for y, c, x, z in every() if c == 0]
TURN = [(flat(y, 1, x, z), flat(z, 1, x, y)) for y, c, x, z in every() if c == 1]


def split(a):
    high = a.astype(jnp.bfloat16)
    return high, (a - high.astype(jnp.float32)).astype(jnp.bfloat16)


def times(turned, b):
    ah, al = split(turned)
    bh, bl = split(b)
    left = jnp.concatenate([ah, ah, al], axis=1)
    right = jnp.concatenate([bh, bl, bh], axis=0)
    return jnp.dot(left, right, preferred_element_type=jnp.float32)


def tile_of(ids_ref, rows_ref, index):
    share, width = rows_ref.shape[1:]
    first = share * index + 1
    row = lax.broadcasted_iota(jnp.int32, (share, width), 0)
    lane = lax.broadcasted_iota(jnp.int32, (share, width), 1)
    tile = jnp.where(lane < first + row, rows_ref[0], 0.0)
    for s in range(ids_ref.shape[0]):
        tile = jnp.where((row == 0) & (lane == first + s), ids_ref[s].astype(jnp.float32), tile)
    return tile


def sent_kernel(ids_ref, left_ref, right_ref, rows_ref, sent_ref, own_ref, held_ref, tile_ref, scratch_ref, sems):
    slots = left_ref.shape[0]
    share, width = rows_ref.shape[1:]
    copies = []
    for s in range(slots):
        pair = (
            pltpu.make_async_copy(left_ref.at[s], scratch_ref.at[s], sems.at[0, s]),
            pltpu.make_async_copy(right_ref.at[s], held_ref.at[s], sems.at[1, s]),
        )
        for copy in pair:
            copy.start()
        copies.append(pair)
    index = lax.axis_index("row")
    core = index % NC
    tile = tile_of(ids_ref, rows_ref, index)
    tile_ref[...] = tile
    for d in range(NY):
        sent_ref[d, slots * share :] = tile
    for s in range(slots):
        for copy in copies[s]:
            copy.wait()
        turned = scratch_ref[s].T.reshape(NY, NC, share, width)
        even, odd = turned[:, 0].reshape(NY * share, width), turned[:, 1].reshape(NY * share, width)
        own_ref[s] = jnp.where(core == 0, even, odd)
        product = times(jnp.where(core == 0, odd, even), held_ref[s])
        sent_ref[:, s * share : (s + 1) * share] = product.reshape(NY, share, width)


def kept_kernel(own_ref, held_ref, tile_ref, kept_ref):
    slots = own_ref.shape[0]
    share, width = tile_ref.shape
    for s in range(slots):
        product = times(own_ref[s], held_ref[s])
        kept_ref[:, s * share : (s + 1) * share] = product.reshape(NY, share, width)
    for d in range(NY):
        kept_ref[d, slots * share :] = tile_ref[...]


def place_kernel(kept_ref, arrived_ref, out_ref):
    for d in range(NY):
        out_ref[d, 0] = kept_ref[d]
        out_ref[d, 1] = arrived_ref[d]


def sum_kernel(got_ref, out_ref, factor_ref, ids_ref, sem):
    share = out_ref.shape[1]
    slots = got_ref.shape[2] // share - 1
    base = slots * share
    copy = pltpu.make_async_copy(got_ref.at[:, :, base : base + 8], ids_ref, sem)
    copy.start()
    index = lax.axis_index("row")
    core = index % NC
    out_ref[...] = jnp.zeros_like(out_ref)

    def first_of(m, half):
        source_core = core if half == 0 else 1 - core
        return share * (jnp.where(core == 0, m, index // NC) * NC + source_core) + 1

    for m in range(NY):
        for half in range(NC):
            tile = got_ref[m, half, base:]
            row = lax.broadcasted_iota(jnp.int32, tile.shape, 0)
            lane = lax.broadcasted_iota(jnp.int32, tile.shape, 1)
            at = (m * NC + half) * share
            factor_ref[at : at + share] = jnp.where(lane < first_of(m, half) + row, tile, 0.0)
    copy.wait()

    def member(m, carry):
        for half in range(NC):
            first = first_of(m, half)
            for s in range(slots):
                k = ids_ref[m, half, 0, first + s].astype(jnp.int32)
                out_ref[k] += got_ref[m, half, s * share : (s + 1) * share]
        return carry

    lax.fori_loop(0, NY, member, 0)


def gram_kernel(factor_ref, own_ref, other_ref, whole_ref):
    whole_ref[...] = times(factor_ref[...].T, factor_ref[...])
    share = own_ref.shape[0]
    start = lax.axis_index("row") // NC * (NC * share)
    own_ref[...] = whole_ref[pl.ds(pl.multiple_of(start, share), share)]
    other_ref[...] = whole_ref[pl.ds(pl.multiple_of(start + share, share), share)]


def on_device(lhat, ainv_anc, diag_inv, targets):
    slots, height, width = lhat.shape
    core = lax.axis_index("row") % NC
    share = diag_inv.shape[1]
    supers = NX * NZ
    length = (slots + 1) * share
    smem, vmem, hbm = (pl.BlockSpec(memory_space=m) for m in (pltpu.SMEM, pltpu.VMEM, pltpu.HBM))

    def here(*lengths):
        return pltpu.VMEM(lengths, jnp.float32)

    def on_chip(x):
        return pltpu.with_memory_space_constraint(x, pltpu.VMEM)

    def call(kernel, ins, outs, mib, *args, scratch=()):
        return pl.pallas_call(
            kernel,
            in_specs=ins,
            out_specs=[vmem] * len(outs),
            out_shape=outs,
            scratch_shapes=scratch,
            compiler_params=pltpu.CompilerParams(vmem_limit_bytes=mib << 20),
            name=kernel.__name__,
        )(*args)

    sent, own, held, tile = call(
        sent_kernel,
        [smem, hbm, hbm, vmem],
        [here(NY, length, width), here(slots, NY * share, width), here(slots, height, width), here(share, width)],
        24,
        targets.reshape(slots),
        pltpu.with_memory_space_constraint(lhat, pltpu.HBM),
        pltpu.with_memory_space_constraint(ainv_anc, pltpu.HBM),
        diag_inv,
        scratch=[pltpu.VMEM((slots, height, width), jnp.float32), pltpu.SemaphoreType.DMA((2, slots))],
    )
    arrived = lax.ppermute(sent, BOTH, PARTNER)
    (kept,) = call(kept_kernel, [vmem] * 3, [here(NY, length, width)], 24, on_chip(own), on_chip(held), on_chip(tile))
    (payload,) = call(place_kernel, [vmem] * 2, [here(NY, NC, length, width)], 24, on_chip(kept), on_chip(arrived))

    got = lax.all_to_all(payload, BOTH, 0, 0, axis_index_groups=LINES, tiled=True)

    summed, factor = call(
        sum_kernel,
        [vmem],
        [here(supers, share, width), here(NY * NC * share, width)],
        24,
        on_chip(got),
        scratch=[pltpu.SMEM((NY, NC, 8, width), jnp.float32), pltpu.SemaphoreType.DMA],
    )

    gram, gram_other = call(
        gram_kernel, [vmem], [here(share, width), here(share, width)], 24, on_chip(factor),
        scratch=[pltpu.VMEM((width, width), jnp.float32)],
    )
    gram_odd = lax.ppermute(gram_other, BOTH, TO_ODD)

    parts = lax.all_to_all(summed, BOTH, 0, 0, axis_index_groups=PLANES, tiled=True)
    total = jnp.sum(parts, axis=0)
    turned = lax.ppermute(total, BOTH, TURN)
    return jnp.where(core == 0, gram - total, gram_odd - turned)[None]


def solution(mesh):
    placed = (
        P(("row", "col"), None, None),
        P(("row", "col"), None, None),
        P("col", "row", None),
        P(("row", "col"), None),
    )
    return jax.shard_map(
        on_device, mesh=mesh, in_specs=placed, out_specs=P("col", "row", None), check_vma=False
    )
```

```python
import jax
import jax.numpy as jnp
from jax import lax
from jax.experimental import pallas as pl
from jax.experimental.pallas import tpu as pltpu
from jax.sharding import PartitionSpec as P

NY, NC, NX, NZ = 8, 2, 4, 8
BOTH = ("row", "col")


def flat(y, c, x, z):
    return ((y * NC + c) * NX + x) * NZ + z


def every():
    return [(y, c, x, z) for y in range(NY) for c in range(NC) for x in range(NX) for z in range(NZ)]


LINES = [[flat(y, 0, x, z) for y in range(NY)] for x in range(NX) for z in range(NZ)] + [
    [flat(y, 1, x, z) for z in range(NZ)] for x in range(NX) for y in range(NY)
]
PLANES = [[flat(y, 0, x, z) for x in range(NX) for z in range(NZ)] for y in range(NY)] + [
    [flat(y, 1, x, z) for x in range(NX) for y in range(NY)] for z in range(NZ)
]
PARTNER = [(flat(y, c, x, z), flat(y, 1 - c, x, z)) for y, c, x, z in every()]
TO_ODD = [(flat(y, 0, x, z), flat(y, 1, x, z)) for y, c, x, z in every() if c == 0]
FAR = NY // 2
TURN = [(flat(y, 1, x, z), flat(z, 1, x, (y + FAR) % NZ)) for y, c, x, z in every() if c == 1]


def split(a):
    high = a.astype(jnp.bfloat16)
    return high, (a - high.astype(jnp.float32)).astype(jnp.bfloat16)


def times(turned, b):
    ah, al = split(turned)
    bh, bl = split(b)
    left = jnp.concatenate([ah, ah, al], axis=1)
    right = jnp.concatenate([bh, bl, bh], axis=0)
    return jnp.dot(left, right, preferred_element_type=jnp.float32)


def tile_of(ids_ref, rows_ref, index):
    share, width = rows_ref.shape[1:]
    first = share * index + 1
    row = lax.broadcasted_iota(jnp.int32, (share, width), 0)
    lane = lax.broadcasted_iota(jnp.int32, (share, width), 1)
    tile = jnp.where(lane < first + row, rows_ref[0], 0.0)
    for s in range(ids_ref.shape[0]):
        tile = jnp.where((row == 0) & (lane == first + s), ids_ref[s].astype(jnp.float32), tile)
    return tile


def sent_kernel(
    ids_hbm, left_ref, right_ref, rows_hbm, sent_ref, own_ref, held_ref, tile_ref, ids_ref, rows_ref, scratch_ref, small, sems
):
    slots = left_ref.shape[0]
    share, width = rows_ref.shape[1:]
    few = (
        pltpu.make_async_copy(ids_hbm, ids_ref, small.at[0]),
        pltpu.make_async_copy(rows_hbm, rows_ref, small.at[1]),
    )
    for copy in few:
        copy.start()
    copies = []
    for s in range(slots):
        pair = (
            pltpu.make_async_copy(left_ref.at[s], scratch_ref.at[s], sems.at[0, s]),
            pltpu.make_async_copy(right_ref.at[s], held_ref.at[s], sems.at[1, s]),
        )
        for copy in pair:
            copy.start()
        copies.append(pair)
    index = lax.axis_index("row")
    core = index % NC
    for copy in few:
        copy.wait()
    tile = tile_of(ids_ref, rows_ref, index)
    tile_ref[...] = tile
    for d in range(NY):
        sent_ref[d, slots * share :] = tile
    for s in range(slots):
        for copy in copies[s]:
            copy.wait()
        turned = scratch_ref[s].T.reshape(NY, NC, share, width)
        even, odd = turned[:, 0].reshape(NY * share, width), turned[:, 1].reshape(NY * share, width)
        own_ref[s] = jnp.where(core == 0, even, odd)
        product = times(jnp.where(core == 0, odd, even), held_ref[s])
        sent_ref[:, s * share : (s + 1) * share] = product.reshape(NY, share, width)


def kept_kernel(own_ref, held_ref, tile_ref, kept_ref):
    slots = own_ref.shape[0]
    share, width = tile_ref.shape
    for s in range(slots):
        product = times(own_ref[s], held_ref[s])
        kept_ref[:, s * share : (s + 1) * share] = product.reshape(NY, share, width)
    for d in range(NY):
        kept_ref[d, slots * share :] = tile_ref[...]


def place_kernel(kept_ref, arrived_ref, out_ref):
    for d in range(NY):
        out_ref[d, 0] = kept_ref[d]
        out_ref[d, 1] = arrived_ref[d]


def sum_kernel(got_ref, out_ref, factor_ref, ids_ref, sem):
    share = out_ref.shape[1]
    slots = got_ref.shape[2] // share - 1
    base = slots * share
    copy = pltpu.make_async_copy(got_ref.at[:, :, base : base + 1], ids_ref, sem)
    copy.start()
    index = lax.axis_index("row")
    core = index % NC
    flip = core * FAR
    out_ref[...] = jnp.zeros_like(out_ref)

    def first_of(m, half):
        source_core = core if half == 0 else 1 - core
        return share * (jnp.where(core == 0, m, index // NC) * NC + source_core) + 1

    for m in range(NY):
        for half in range(NC):
            tile = got_ref[m, half, base:]
            row = lax.broadcasted_iota(jnp.int32, tile.shape, 0)
            lane = lax.broadcasted_iota(jnp.int32, tile.shape, 1)
            at = (m * NC + half) * share
            factor_ref[at : at + share] = jnp.where(lane < first_of(m, half) + row, tile, 0.0)
    copy.wait()

    def member(m, carry):
        for half in range(NC):
            first = first_of(m, half)
            for s in range(slots):
                k = ids_ref[m, half, 0, first + s].astype(jnp.int32)
                out_ref[k ^ flip] += got_ref[m, half, s * share : (s + 1) * share]
        return carry

    lax.fori_loop(0, NY, member, 0)


def gram_kernel(factor_ref, own_ref, other_ref, whole_ref):
    whole_ref[...] = times(factor_ref[...].T, factor_ref[...])
    share = own_ref.shape[0]
    start = lax.axis_index("row") // NC * (NC * share)
    own_ref[...] = whole_ref[pl.ds(pl.multiple_of(start, share), share)]
    other_ref[...] = whole_ref[pl.ds(pl.multiple_of(start + share, share), share)]


def on_device(lhat, ainv_anc, diag_inv, targets):
    slots, height, width = lhat.shape
    core = lax.axis_index("row") % NC
    share = diag_inv.shape[1]
    supers = NX * NZ
    length = (slots + 1) * share
    vmem, hbm = (pl.BlockSpec(memory_space=m) for m in (pltpu.VMEM, pltpu.HBM))

    def here(*lengths):
        return pltpu.VMEM(lengths, jnp.float32)

    def on_chip(x):
        return pltpu.with_memory_space_constraint(x, pltpu.VMEM)

    def call(kernel, ins, outs, mib, *args, scratch=()):
        return pl.pallas_call(
            kernel,
            in_specs=ins,
            out_specs=[vmem] * len(outs),
            out_shape=outs,
            scratch_shapes=scratch,
            compiler_params=pltpu.CompilerParams(vmem_limit_bytes=mib << 20),
            name=kernel.__name__,
        )(*args)

    sent, own, held, tile = call(
        sent_kernel,
        [hbm] * 4,
        [here(NY, length, width), here(slots, NY * share, width), here(slots, height, width), here(share, width)],
        24,
        *(
            pltpu.with_memory_space_constraint(x, pltpu.HBM)
            for x in (targets.reshape(slots), lhat, ainv_anc, diag_inv)
        ),
        scratch=[
            pltpu.SMEM((slots,), jnp.int32),
            pltpu.VMEM((1, share, width), jnp.float32),
            pltpu.VMEM((slots, height, width), jnp.float32),
            pltpu.SemaphoreType.DMA((2,)),
            pltpu.SemaphoreType.DMA((2, slots)),
        ],
    )
    arrived = lax.ppermute(sent, BOTH, PARTNER)
    (kept,) = call(kept_kernel, [vmem] * 3, [here(NY, length, width)], 24, on_chip(own), on_chip(held), on_chip(tile))
    (payload,) = call(place_kernel, [vmem] * 2, [here(NY, NC, length, width)], 24, on_chip(kept), on_chip(arrived))

    got = lax.all_to_all(payload, BOTH, 0, 0, axis_index_groups=LINES, tiled=True)

    summed, factor = call(
        sum_kernel,
        [vmem],
        [here(supers, share, width), here(NY * NC * share, width)],
        24,
        on_chip(got),
        scratch=[pltpu.SMEM((NY, NC, 1, width), jnp.float32), pltpu.SemaphoreType.DMA],
    )

    gram, gram_other = call(
        gram_kernel, [vmem], [here(share, width), here(share, width)], 24, on_chip(factor),
        scratch=[pltpu.VMEM((width, width), jnp.float32)],
    )
    gram_odd = lax.ppermute(gram_other, BOTH, TO_ODD)

    parts = lax.all_to_all(summed, BOTH, 0, 0, axis_index_groups=PLANES, tiled=True)
    total = jnp.sum(parts, axis=0)
    turned = lax.ppermute(total, BOTH, TURN)
    return jnp.where(core == 0, gram - total, gram_odd - turned)[None]


def solution(mesh):
    placed = (
        P(("row", "col"), None, None),
        P(("row", "col"), None, None),
        P("col", "row", None),
        P(("row", "col"), None),
    )
    return jax.shard_map(
        on_device, mesh=mesh, in_specs=placed, out_specs=P("col", "row", None), check_vma=False
    )
```

```python
import jax
import jax.numpy as jnp
from jax import lax
from jax.experimental import pallas as pl
from jax.experimental.pallas import tpu as pltpu
from jax.sharding import PartitionSpec as P


NY, NC, NX, NZ = 8, 2, 4, 8
BOTH = ("row", "col")


def flat(y, c, x, z):
    return ((y * NC + c) * NX + x) * NZ + z


def every():
    return [(y, c, x, z) for y in range(NY) for c in range(NC) for x in range(NX) for z in range(NZ)]


LINES = [[flat(y, 0, x, z) for y in range(NY)] for x in range(NX) for z in range(NZ)] + [
    [flat(y, 1, x, z) for z in range(NZ)] for x in range(NX) for y in range(NY)
]
PLANES = [[flat(y, 0, x, z) for x in range(NX) for z in range(NZ)] for y in range(NY)] + [
    [flat(y, 1, x, z) for x in range(NX) for y in range(NY)] for z in range(NZ)
]
PARTNER = [(flat(y, c, x, z), flat(y, 1 - c, x, z)) for y, c, x, z in every()]
TO_ODD = [(flat(y, 0, x, z), flat(y, 1, x, z)) for y, c, x, z in every() if c == 0]
FAR = NY // 2
TURN = [(flat(y, 1, x, z), flat(z, 1, x, (y + FAR) % NZ)) for y, c, x, z in every() if c == 1]


def split(a):
    high = a.astype(jnp.bfloat16)
    return high, (a - high.astype(jnp.float32)).astype(jnp.bfloat16)


def times(turned, b):
    ah, al = turned
    bh, bl = split(b)
    left = jnp.concatenate([ah, ah, al], axis=1)
    right = jnp.concatenate([bh, bl, bh], axis=0)
    return jnp.dot(left, right, preferred_element_type=jnp.float32)


def tile_of(ids_ref, rows_ref, index):
    share, width = rows_ref.shape[1:]
    first = share * index + 1
    row = lax.broadcasted_iota(jnp.int32, (share, width), 0)
    lane = lax.broadcasted_iota(jnp.int32, (share, width), 1)
    tile = jnp.where(lane < first + row, rows_ref[0], 0.0)
    for s in range(ids_ref.shape[0]):
        tile = jnp.where((row == 0) & (lane == first + s), ids_ref[s].astype(jnp.float32), tile)
    return tile


def sent_kernel(
    ids_hbm, left_ref, right_ref, rows_hbm, sent_ref, own_ref, held_ref, tile_ref, ids_ref, rows_ref, scratch_ref, small, sems
):
    slots = left_ref.shape[0]
    share, width = rows_ref.shape[1:]
    few = (
        pltpu.make_async_copy(ids_hbm, ids_ref, small.at[0]),
        pltpu.make_async_copy(rows_hbm, rows_ref, small.at[1]),
    )
    for copy in few:
        copy.start()
    copies = []
    for s in range(slots):
        pair = (
            pltpu.make_async_copy(left_ref.at[s], scratch_ref.at[s], sems.at[0, s]),
            pltpu.make_async_copy(right_ref.at[s], held_ref.at[s], sems.at[1, s]),
        )
        for copy in pair:
            copy.start()
        copies.append(pair)
    index = lax.axis_index("row")
    core = index % NC
    for s in range(slots):
        for copy in copies[s]:
            copy.wait()
        parts = []
        for i, part in enumerate(split(scratch_ref[s])):
            part = part.T.reshape(NY, NC, share, width)
            even, odd = part[:, 0].reshape(NY * share, width), part[:, 1].reshape(NY * share, width)
            own_ref[i, s] = jnp.where(core == 0, even, odd)
            parts.append(jnp.where(core == 0, odd, even))
        product = times(parts, held_ref[s])
        sent_ref[:, s * share : (s + 1) * share] = product.reshape(NY, share, width)
    for copy in few:
        copy.wait()
    tile = tile_of(ids_ref, rows_ref, index)
    tile_ref[...] = tile
    for d in range(NY):
        sent_ref[d, slots * share :] = tile


def kept_kernel(own_ref, held_ref, tile_ref, kept_ref):
    slots = held_ref.shape[0]
    share, width = tile_ref.shape
    for s in range(slots):
        product = times((own_ref[0, s], own_ref[1, s]), held_ref[s])
        kept_ref[:, s * share : (s + 1) * share] = product.reshape(NY, share, width)
    for d in range(NY):
        kept_ref[d, slots * share :] = tile_ref[...]


def place_kernel(kept_ref, arrived_ref, out_ref):
    for d in range(NY):
        out_ref[d, 0] = kept_ref[d]
        out_ref[d, 1] = arrived_ref[d]


def sum_kernel(got_ref, out_ref, factor_ref, ids_ref, sem):
    share = out_ref.shape[1]
    slots = got_ref.shape[2] // share - 1
    base = slots * share
    copy = pltpu.make_async_copy(got_ref.at[:, :, base : base + 1], ids_ref, sem)
    copy.start()
    index = lax.axis_index("row")
    core = index % NC
    flip = core * FAR
    out_ref[...] = jnp.zeros_like(out_ref)

    def first_of(m, half):
        source_core = core if half == 0 else 1 - core
        return share * (jnp.where(core == 0, m, index // NC) * NC + source_core) + 1

    for m in range(NY):
        for half in range(NC):
            tile = got_ref[m, half, base:]
            row = lax.broadcasted_iota(jnp.int32, tile.shape, 0)
            lane = lax.broadcasted_iota(jnp.int32, tile.shape, 1)
            at = (m * NC + half) * share
            factor_ref[at : at + share] = jnp.where(lane < first_of(m, half) + row, tile, 0.0)
    copy.wait()

    def member(m, carry):
        for half in range(NC):
            first = first_of(m, half)
            for s in range(slots):
                k = ids_ref[m, half, 0, first + s].astype(jnp.int32)
                out_ref[k ^ flip] += got_ref[m, half, s * share : (s + 1) * share]
        return carry

    lax.fori_loop(0, NY, member, 0)


def gram_kernel(factor_ref, own_ref, other_ref, whole_ref):
    whole_ref[...] = times(split(factor_ref[...].T), factor_ref[...])
    share = own_ref.shape[0]
    start = lax.axis_index("row") // NC * (NC * share)
    own_ref[...] = whole_ref[pl.ds(pl.multiple_of(start, share), share)]
    other_ref[...] = whole_ref[pl.ds(pl.multiple_of(start + share, share), share)]


def on_device(lhat, ainv_anc, diag_inv, targets):
    slots, height, width = lhat.shape
    core = lax.axis_index("row") % NC
    share = diag_inv.shape[1]
    supers = NX * NZ
    length = (slots + 1) * share
    vmem, hbm = (pl.BlockSpec(memory_space=m) for m in (pltpu.VMEM, pltpu.HBM))

    def here(*lengths, dtype=jnp.float32):
        return pltpu.VMEM(lengths, dtype)

    def on_chip(x):
        return pltpu.with_memory_space_constraint(x, pltpu.VMEM)

    def call(kernel, ins, outs, mib, *args, scratch=()):
        return pl.pallas_call(
            kernel,
            in_specs=ins,
            out_specs=[vmem] * len(outs),
            out_shape=outs,
            scratch_shapes=scratch,
            compiler_params=pltpu.CompilerParams(vmem_limit_bytes=mib << 20),
        )(*args)

    sent, own, held, tile = call(
        sent_kernel,
        [hbm] * 4,
        [
            here(NY, length, width),
            here(2, slots, NY * share, width, dtype=jnp.bfloat16),
            here(slots, height, width),
            here(share, width),
        ],
        24,
        *(
            pltpu.with_memory_space_constraint(x, pltpu.HBM)
            for x in (targets.reshape(slots), lhat, ainv_anc, diag_inv)
        ),
        scratch=[
            pltpu.SMEM((slots,), jnp.int32),
            pltpu.VMEM((1, share, width), jnp.float32),
            pltpu.VMEM((slots, height, width), jnp.float32),
            pltpu.SemaphoreType.DMA((2,)),
            pltpu.SemaphoreType.DMA((2, slots)),
        ],
    )
    arrived = lax.ppermute(sent, BOTH, PARTNER)
    (kept,) = call(kept_kernel, [vmem] * 3, [here(NY, length, width)], 24, on_chip(own), on_chip(held), on_chip(tile))
    (payload,) = call(place_kernel, [vmem] * 2, [here(NY, NC, length, width)], 24, on_chip(kept), on_chip(arrived))

    got = lax.all_to_all(payload, BOTH, 0, 0, axis_index_groups=LINES, tiled=True)

    summed, factor = call(
        sum_kernel,
        [vmem],
        [here(supers, share, width), here(NY * NC * share, width)],
        24,
        on_chip(got),
        scratch=[pltpu.SMEM((NY, NC, 1, width), jnp.float32), pltpu.SemaphoreType.DMA],
    )

    parts = lax.all_to_all(summed, BOTH, 0, 0, axis_index_groups=PLANES, tiled=True)
    total = jnp.sum(parts, axis=0)
    turned = lax.ppermute(total, BOTH, TURN)

    factor, total = lax.optimization_barrier((factor, total))
    gram, gram_other = call(
        gram_kernel, [vmem], [here(share, width), here(share, width)], 24, on_chip(factor),
        scratch=[pltpu.VMEM((width, width), jnp.float32)],
    )
    gram_odd = lax.ppermute(gram_other, BOTH, TO_ODD)
    return jnp.where(core == 0, gram - total, gram_odd - turned)[None]


def solution(mesh):
    placed = (
        P(("row", "col"), None, None),
        P(("row", "col"), None, None),
        P("col", "row", None),
        P(("row", "col"), None),
    )
    return jax.shard_map(
        on_device, mesh=mesh, in_specs=placed, out_specs=P("col", "row", None), check_vma=False
    )
```

```python
import jax
import jax.numpy as jnp
from jax import lax
from jax.experimental import pallas as pl
from jax.experimental.pallas import tpu as pltpu
from jax.sharding import PartitionSpec as P


NY, NC, NX, NZ = 8, 2, 4, 8
BOTH = ("row", "col")


def flat(y, c, x, z):
    return ((y * NC + c) * NX + x) * NZ + z


def every():
    return [(y, c, x, z) for y in range(NY) for c in range(NC) for x in range(NX) for z in range(NZ)]


PLANES = [[flat(y, 0, x, z) for x in range(NX) for z in range(NZ)] for y in range(NY)] + [
    [flat(y, 1, x, z) for x in range(NX) for y in range(NY)] for z in range(NZ)
]
SHIFTS = (4, 3, 5, 2, 6, 1, 7)
EARLY = 4


def along(shift):
    return [
        (flat(y, c, x, z), flat((y + shift) % NY, 0, x, z) if c == 0 else flat(y, 1, x, (z + shift) % NZ))
        for y, c, x, z in every()
    ]


PARTNER = [(flat(y, c, x, z), flat(y, 1 - c, x, z)) for y, c, x, z in every()]
TO_ODD = [(flat(y, 0, x, z), flat(y, 1, x, z)) for y, c, x, z in every() if c == 0]
FAR = NY // 2
TURN = [(flat(y, 1, x, z), flat(z, 1, x, (y + FAR) % NZ)) for y, c, x, z in every() if c == 1]


def split(a):
    high = a.astype(jnp.bfloat16)
    return high, (a - high.astype(jnp.float32)).astype(jnp.bfloat16)


def times(turned, b):
    ah, al = turned
    bh, bl = split(b)
    left = jnp.concatenate([ah, ah, al], axis=1)
    right = jnp.concatenate([bh, bl, bh], axis=0)
    return jnp.dot(left, right, preferred_element_type=jnp.float32)


def tile_of(ids_ref, rows_ref, index):
    share, width = rows_ref.shape[1:]
    first = share * index + 1
    row = lax.broadcasted_iota(jnp.int32, (share, width), 0)
    lane = lax.broadcasted_iota(jnp.int32, (share, width), 1)
    tile = jnp.where(lane < first + row, rows_ref[0], 0.0)
    for s in range(ids_ref.shape[0]):
        tile = jnp.where((row == 0) & (lane == first + s), ids_ref[s].astype(jnp.float32), tile)
    return tile


def sent_kernel(
    ids_hbm, left_ref, right_ref, rows_hbm, sent_ref, own_ref, held_ref, tile_ref, ids_ref, rows_ref, scratch_ref, small, sems
):
    slots = left_ref.shape[0]
    share, width = rows_ref.shape[1:]
    few = (
        pltpu.make_async_copy(ids_hbm, ids_ref, small.at[0]),
        pltpu.make_async_copy(rows_hbm, rows_ref, small.at[1]),
    )
    for copy in few:
        copy.start()
    copies = []
    for s in range(slots):
        pair = (
            pltpu.make_async_copy(left_ref.at[s], scratch_ref.at[s], sems.at[0, s]),
            pltpu.make_async_copy(right_ref.at[s], held_ref.at[s], sems.at[1, s]),
        )
        for copy in pair:
            copy.start()
        copies.append(pair)
    index = lax.axis_index("row")
    core = index % NC
    for s in range(slots):
        for copy in copies[s]:
            copy.wait()
        parts = []
        for i, part in enumerate(split(scratch_ref[s])):
            part = part.T.reshape(NY, NC, share, width)
            even, odd = part[:, 0].reshape(NY * share, width), part[:, 1].reshape(NY * share, width)
            own_ref[i, s] = jnp.where(core == 0, even, odd)
            parts.append(jnp.where(core == 0, odd, even))
        product = times(parts, held_ref[s])
        sent_ref[:, s * share : (s + 1) * share] = product.reshape(NY, share, width)
    for copy in few:
        copy.wait()
    tile = tile_of(ids_ref, rows_ref, index)
    tile_ref[...] = tile
    for d in range(NY):
        sent_ref[d, slots * share :] = tile


def kept_kernel(own_ref, held_ref, tile_ref, kept_ref):
    slots = held_ref.shape[0]
    share, width = tile_ref.shape
    for s in range(slots):
        product = times((own_ref[0, s], own_ref[1, s]), held_ref[s])
        kept_ref[:, s * share : (s + 1) * share] = product.reshape(NY, share, width)
    for d in range(NY):
        kept_ref[d, slots * share :] = tile_ref[...]


def place_kernel(kept_ref, arrived_ref, *out_refs):
    index = lax.axis_index("row")
    me = jnp.where(index % NC == 0, index // NC, lax.axis_index("col") % NZ)
    for shift, out_ref in zip((0, *SHIFTS), out_refs):
        out_ref[0] = kept_ref[(me + shift) % NY]
        out_ref[1] = arrived_ref[(me + shift) % NY]


def add_blocks(shifts, got_refs, ids_refs, sems, out_ref, factor_ref):
    share = out_ref.shape[1]
    slots = got_refs[0].shape[1] // share - 1
    base = slots * share
    copies = [
        pltpu.make_async_copy(got_ref.at[:, base : base + 1], ids_ref, sems.at[i])
        for i, (got_ref, ids_ref) in enumerate(zip(got_refs, ids_refs))
    ]
    for copy in copies:
        copy.start()
    index = lax.axis_index("row")
    core = index % NC
    flip = core * FAR

    def first_of(shift, half):
        source_core = core if half == 0 else 1 - core
        return share * (jnp.where(core == 0, (index // NC + NY - shift) % NY, index // NC) * NC + source_core) + 1

    for shift, got_ref in zip(shifts, got_refs):
        source = (index // NC + NY - shift) % NY
        for half in range(NC):
            tile = got_ref[half, base:]
            row = lax.broadcasted_iota(jnp.int32, tile.shape, 0)
            lane = lax.broadcasted_iota(jnp.int32, tile.shape, 1)
            at = pl.multiple_of((source * NC + half) * share, share)
            factor_ref[pl.ds(at, share)] = jnp.where(lane < first_of(shift, half) + row, tile, 0.0)
    for copy in copies:
        copy.wait()
    for shift, got_ref, ids_ref in zip(shifts, got_refs, ids_refs):
        for half in range(NC):
            first = first_of(shift, half)
            for s in range(slots):
                k = ids_ref[half, 0, first + s].astype(jnp.int32)
                out_ref[k ^ flip] += got_ref[half, s * share : (s + 1) * share]


def early_kernel(*refs):
    n = EARLY + 1
    got_refs, (out_ref, factor_ref), ids_refs, sems = refs[:n], refs[n : n + 2], refs[n + 2 : -1], refs[-1]
    out_ref[...] = jnp.zeros_like(out_ref)
    factor_ref[...] = jnp.zeros_like(factor_ref)
    add_blocks((0, *SHIFTS[:EARLY]), got_refs, ids_refs, sems, out_ref, factor_ref)


def late_kernel(sum_ref, rows_ref, *refs):
    n = len(SHIFTS) - EARLY
    got_refs, (out_ref, factor_ref), ids_refs, sems = refs[:n], refs[n : n + 2], refs[n + 2 : -1], refs[-1]
    out_ref[...] = sum_ref[...]
    factor_ref[...] = rows_ref[...]
    add_blocks(SHIFTS[EARLY:], got_refs, ids_refs, sems, out_ref, factor_ref)


def gram_kernel(factor_ref, own_ref, other_ref, whole_ref):
    whole_ref[...] = times(split(factor_ref[...].T), factor_ref[...])
    share = own_ref.shape[0]
    start = lax.axis_index("row") // NC * (NC * share)
    own_ref[...] = whole_ref[pl.ds(pl.multiple_of(start, share), share)]
    other_ref[...] = whole_ref[pl.ds(pl.multiple_of(start + share, share), share)]


def on_device(lhat, ainv_anc, diag_inv, targets):
    slots, height, width = lhat.shape
    core = lax.axis_index("row") % NC
    share = diag_inv.shape[1]
    supers = NX * NZ
    length = (slots + 1) * share
    vmem, hbm = (pl.BlockSpec(memory_space=m) for m in (pltpu.VMEM, pltpu.HBM))

    def here(*lengths, dtype=jnp.float32):
        return pltpu.VMEM(lengths, dtype)

    def on_chip(x):
        return pltpu.with_memory_space_constraint(x, pltpu.VMEM)

    def call(kernel, ins, outs, mib, *args, scratch=()):
        return pl.pallas_call(
            kernel,
            in_specs=ins,
            out_specs=[vmem] * len(outs),
            out_shape=outs,
            scratch_shapes=scratch,
            compiler_params=pltpu.CompilerParams(vmem_limit_bytes=mib << 20),
        )(*args)

    sent, own, held, tile = call(
        sent_kernel,
        [hbm] * 4,
        [
            here(NY, length, width),
            here(2, slots, NY * share, width, dtype=jnp.bfloat16),
            here(slots, height, width),
            here(share, width),
        ],
        24,
        *(
            pltpu.with_memory_space_constraint(x, pltpu.HBM)
            for x in (targets.reshape(slots), lhat, ainv_anc, diag_inv)
        ),
        scratch=[
            pltpu.SMEM((slots,), jnp.int32),
            pltpu.VMEM((1, share, width), jnp.float32),
            pltpu.VMEM((slots, height, width), jnp.float32),
            pltpu.SemaphoreType.DMA((2,)),
            pltpu.SemaphoreType.DMA((2, slots)),
        ],
    )
    arrived = lax.ppermute(sent, BOTH, PARTNER)
    (kept,) = call(kept_kernel, [vmem] * 3, [here(NY, length, width)], 24, on_chip(own), on_chip(held), on_chip(tile))
    own_message, *messages = call(
        place_kernel,
        [vmem] * 2,
        [here(NC, length, width)] * NY,
        24,
        on_chip(kept),
        on_chip(arrived),
    )
    got = [lax.ppermute(message, BOTH, along(shift)) for message, shift in zip(messages, SHIFTS)]

    def numbers(n):
        return [pltpu.SMEM((NC, 1, width), jnp.float32)] * n + [pltpu.SemaphoreType.DMA((n,))]

    results = [here(supers, share, width), here(NY * NC * share, width)]
    partial = call(
        early_kernel,
        [vmem] * (EARLY + 1),
        results,
        24,
        *(on_chip(x) for x in (own_message, *got[:EARLY])),
        scratch=numbers(EARLY + 1),
    )
    summed, factor = call(
        late_kernel,
        [vmem] * (2 + len(SHIFTS) - EARLY),
        results,
        24,
        *(on_chip(x) for x in (*partial, *got[EARLY:])),
        scratch=numbers(len(SHIFTS) - EARLY),
    )

    parts = lax.all_to_all(summed, BOTH, 0, 0, axis_index_groups=PLANES, tiled=True)
    total = jnp.sum(parts, axis=0)
    turned = lax.ppermute(total, BOTH, TURN)

    factor, total = lax.optimization_barrier((factor, total))
    gram, gram_other = call(
        gram_kernel, [vmem], [here(share, width), here(share, width)], 24, on_chip(factor),
        scratch=[pltpu.VMEM((width, width), jnp.float32)],
    )
    gram_odd = lax.ppermute(gram_other, BOTH, TO_ODD)
    return jnp.where(core == 0, gram - total, gram_odd - turned)[None]


def solution(mesh):
    placed = (
        P(("row", "col"), None, None),
        P(("row", "col"), None, None),
        P("col", "row", None),
        P(("row", "col"), None),
    )
    return jax.shard_map(
        on_device, mesh=mesh, in_specs=placed, out_specs=P("col", "row", None), check_vma=False
    )
```

```python
import jax
import jax.numpy as jnp
from jax import lax
from jax.experimental import pallas as pl
from jax.experimental.pallas import tpu as pltpu
from jax.sharding import PartitionSpec as P


NY, NC, NX, NZ = 8, 2, 4, 8
BOTH = ("row", "col")


def flat(y, c, x, z):
    return ((y * NC + c) * NX + x) * NZ + z


def every():
    return [(y, c, x, z) for y in range(NY) for c in range(NC) for x in range(NX) for z in range(NZ)]


PLANES = [[flat(y, 0, x, z) for x in range(NX) for z in range(NZ)] for y in range(NY)] + [
    [flat(y, 1, x, z) for x in range(NX) for y in range(NY)] for z in range(NZ)
]
SHIFTS = (4, 3, 5, 2, 6, 1, 7)
EARLY = 5


def along(shift):
    return [
        (flat(y, c, x, z), flat((y + shift) % NY, 0, x, z) if c == 0 else flat(y, 1, x, (z + shift) % NZ))
        for y, c, x, z in every()
    ]


PARTNER = [(flat(y, c, x, z), flat(y, 1 - c, x, z)) for y, c, x, z in every()]
TO_ODD = [(flat(y, 0, x, z), flat(y, 1, x, z)) for y, c, x, z in every() if c == 0]
FAR = NY // 2
TURN = [(flat(y, 1, x, z), flat(z, 1, x, (y + FAR) % NZ)) for y, c, x, z in every() if c == 1]


def split(a):
    high = a.astype(jnp.bfloat16)
    return high, (a - high.astype(jnp.float32)).astype(jnp.bfloat16)


def times(turned, b):
    ah, al = turned
    bh, bl = split(b)
    left = jnp.concatenate([ah, ah, al], axis=1)
    right = jnp.concatenate([bh, bl, bh], axis=0)
    return jnp.dot(left, right, preferred_element_type=jnp.float32)


def tile_of(ids_ref, rows_ref, index):
    share, width = rows_ref.shape[1:]
    first = share * index + 1
    row = lax.broadcasted_iota(jnp.int32, (share, width), 0)
    lane = lax.broadcasted_iota(jnp.int32, (share, width), 1)
    tile = jnp.where(lane < first + row, rows_ref[0], 0.0)
    for s in range(ids_ref.shape[0]):
        tile = jnp.where((row == 0) & (lane == first + s), ids_ref[s].astype(jnp.float32), tile)
    return tile


def sent_kernel(
    ids_hbm, left_ref, right_ref, rows_hbm, sent_ref, own_ref, held_ref, tile_ref, ids_ref, rows_ref, scratch_ref, small, sems
):
    slots = left_ref.shape[0]
    share, width = rows_ref.shape[1:]
    few = (
        pltpu.make_async_copy(ids_hbm, ids_ref, small.at[0]),
        pltpu.make_async_copy(rows_hbm, rows_ref, small.at[1]),
    )
    for copy in few:
        copy.start()
    copies = []
    for s in range(slots):
        pair = (
            pltpu.make_async_copy(left_ref.at[s], scratch_ref.at[s], sems.at[0, s]),
            pltpu.make_async_copy(right_ref.at[s], held_ref.at[s], sems.at[1, s]),
        )
        for copy in pair:
            copy.start()
        copies.append(pair)
    index = lax.axis_index("row")
    core = index % NC
    for s in range(slots):
        for copy in copies[s]:
            copy.wait()
        parts = []
        for i, part in enumerate(split(scratch_ref[s])):
            part = part.T.reshape(NY, NC, share, width)
            even, odd = part[:, 0].reshape(NY * share, width), part[:, 1].reshape(NY * share, width)
            own_ref[i, s] = jnp.where(core == 0, even, odd)
            parts.append(jnp.where(core == 0, odd, even))
        product = times(parts, held_ref[s])
        sent_ref[:, s * share : (s + 1) * share] = product.reshape(NY, share, width)
    for copy in few:
        copy.wait()
    tile = tile_of(ids_ref, rows_ref, index)
    tile_ref[...] = tile
    for d in range(NY):
        sent_ref[d, slots * share :] = tile


def kept_kernel(own_ref, held_ref, tile_ref, kept_ref):
    slots = held_ref.shape[0]
    share, width = tile_ref.shape
    for s in range(slots):
        product = times((own_ref[0, s], own_ref[1, s]), held_ref[s])
        kept_ref[:, s * share : (s + 1) * share] = product.reshape(NY, share, width)
    for d in range(NY):
        kept_ref[d, slots * share :] = tile_ref[...]


def place_kernel(kept_ref, arrived_ref, *out_refs):
    index = lax.axis_index("row")
    me = jnp.where(index % NC == 0, index // NC, lax.axis_index("col") % NZ)
    for shift, out_ref in zip((0, *SHIFTS), out_refs):
        out_ref[0] = kept_ref[(me + shift) % NY]
        out_ref[1] = arrived_ref[(me + shift) % NY]


def add_blocks(shifts, got_refs, ids_refs, sems, out_ref, factor_ref, summed, rows):
    share = out_ref.shape[1]
    slots = got_refs[0].shape[1] // share - 1
    base = slots * share
    copies = [
        pltpu.make_async_copy(got_ref.at[:, base : base + 1], ids_ref, sems.at[i])
        for i, (got_ref, ids_ref) in enumerate(zip(got_refs, ids_refs))
    ]
    for copy in copies:
        copy.start()
    out_ref[...] = summed()
    factor_ref[...] = rows()
    index = lax.axis_index("row")
    core = index % NC
    flip = core * FAR

    def first_of(shift, half):
        source_core = core if half == 0 else 1 - core
        return share * (jnp.where(core == 0, (index // NC + NY - shift) % NY, index // NC) * NC + source_core) + 1

    for shift, got_ref in zip(shifts, got_refs):
        source = (index // NC + NY - shift) % NY
        for half in range(NC):
            tile = got_ref[half, base:]
            row = lax.broadcasted_iota(jnp.int32, tile.shape, 0)
            lane = lax.broadcasted_iota(jnp.int32, tile.shape, 1)
            at = pl.multiple_of((source * NC + half) * share, share)
            factor_ref[pl.ds(at, share)] = jnp.where(lane < first_of(shift, half) + row, tile, 0.0)
    for copy in copies:
        copy.wait()
    for shift, got_ref, ids_ref in zip(shifts, got_refs, ids_refs):
        for half in range(NC):
            first = first_of(shift, half)
            for s in range(slots):
                k = ids_ref[half, 0, first + s].astype(jnp.int32)
                out_ref[k ^ flip] += got_ref[half, s * share : (s + 1) * share]


def early_kernel(*refs):
    n = EARLY + 1
    got_refs, (out_ref, factor_ref), ids_refs, sems = refs[:n], refs[n : n + 2], refs[n + 2 : -1], refs[-1]
    zeros = (lambda: jnp.zeros_like(out_ref), lambda: jnp.zeros_like(factor_ref))
    add_blocks((0, *SHIFTS[:EARLY]), got_refs, ids_refs, sems, out_ref, factor_ref, *zeros)


def late_kernel(sum_ref, rows_ref, *refs):
    n = len(SHIFTS) - EARLY
    got_refs, (out_ref, factor_ref), ids_refs, sems = refs[:n], refs[n : n + 2], refs[n + 2 : -1], refs[-1]
    before = (lambda: sum_ref[...], lambda: rows_ref[...])
    add_blocks(SHIFTS[EARLY:], got_refs, ids_refs, sems, out_ref, factor_ref, *before)


def gram_kernel(factor_ref, own_ref, other_ref, whole_ref):
    whole_ref[...] = times(split(factor_ref[...].T), factor_ref[...])
    share = own_ref.shape[0]
    start = lax.axis_index("row") // NC * (NC * share)
    own_ref[...] = whole_ref[pl.ds(pl.multiple_of(start, share), share)]
    other_ref[...] = whole_ref[pl.ds(pl.multiple_of(start + share, share), share)]


def on_device(lhat, ainv_anc, diag_inv, targets):
    slots, height, width = lhat.shape
    core = lax.axis_index("row") % NC
    share = diag_inv.shape[1]
    supers = NX * NZ
    length = (slots + 1) * share
    vmem, hbm = (pl.BlockSpec(memory_space=m) for m in (pltpu.VMEM, pltpu.HBM))

    def here(*lengths, dtype=jnp.float32):
        return pltpu.VMEM(lengths, dtype)

    def on_chip(x):
        return pltpu.with_memory_space_constraint(x, pltpu.VMEM)

    def call(kernel, ins, outs, mib, *args, scratch=()):
        return pl.pallas_call(
            kernel,
            in_specs=ins,
            out_specs=[vmem] * len(outs),
            out_shape=outs,
            scratch_shapes=scratch,
            compiler_params=pltpu.CompilerParams(vmem_limit_bytes=mib << 20),
        )(*args)

    sent, own, held, tile = call(
        sent_kernel,
        [hbm] * 4,
        [
            here(NY, length, width),
            here(2, slots, NY * share, width, dtype=jnp.bfloat16),
            here(slots, height, width),
            here(share, width),
        ],
        24,
        *(
            pltpu.with_memory_space_constraint(x, pltpu.HBM)
            for x in (targets.reshape(slots), lhat, ainv_anc, diag_inv)
        ),
        scratch=[
            pltpu.SMEM((slots,), jnp.int32),
            pltpu.VMEM((1, share, width), jnp.float32),
            pltpu.VMEM((slots, height, width), jnp.float32),
            pltpu.SemaphoreType.DMA((2,)),
            pltpu.SemaphoreType.DMA((2, slots)),
        ],
    )
    arrived = lax.ppermute(sent, BOTH, PARTNER)
    (kept,) = call(kept_kernel, [vmem] * 3, [here(NY, length, width)], 24, on_chip(own), on_chip(held), on_chip(tile))
    own_message, *messages = call(
        place_kernel,
        [vmem] * 2,
        [here(NC, length, width)] * NY,
        24,
        on_chip(kept),
        on_chip(arrived),
    )
    got = [lax.ppermute(message, BOTH, along(shift)) for message, shift in zip(messages, SHIFTS)]

    def numbers(n):
        return [pltpu.SMEM((NC, 1, width), jnp.float32)] * n + [pltpu.SemaphoreType.DMA((n,))]

    results = [here(supers, share, width), here(NY * NC * share, width)]
    partial = call(
        early_kernel,
        [vmem] * (EARLY + 1),
        results,
        24,
        *(on_chip(x) for x in (own_message, *got[:EARLY])),
        scratch=numbers(EARLY + 1),
    )
    summed, factor = call(
        late_kernel,
        [vmem] * (2 + len(SHIFTS) - EARLY),
        results,
        24,
        *(on_chip(x) for x in (*partial, *got[EARLY:])),
        scratch=numbers(len(SHIFTS) - EARLY),
    )

    parts = lax.all_to_all(summed, BOTH, 0, 0, axis_index_groups=PLANES, tiled=True)
    total = jnp.sum(parts, axis=0)
    turned = lax.ppermute(total, BOTH, TURN)

    factor, total = lax.optimization_barrier((factor, total))
    gram, gram_other = call(
        gram_kernel, [vmem], [here(share, width), here(share, width)], 24, on_chip(factor),
        scratch=[pltpu.VMEM((width, width), jnp.float32)],
    )
    gram_odd = lax.ppermute(gram_other, BOTH, TO_ODD)
    return jnp.where(core == 0, gram - total, gram_odd - turned)[None]


def solution(mesh):
    placed = (
        P(("row", "col"), None, None),
        P(("row", "col"), None, None),
        P("col", "row", None),
        P(("row", "col"), None),
    )
    return jax.shard_map(
        on_device, mesh=mesh, in_specs=placed, out_specs=P("col", "row", None), check_vma=False
    )
```
